32 devices in a mesh: fsdp: 8 (over z, y), seq: 4 (over x, core).
Axes of the slice: x: 2, y: 2, z: 4, core: 2. Of those that a mesh axis runs over, the one named last changes fastest.
Arguments:
- tokens: bfloat16 [8, 512, 4096], P('fsdp'), may hold values from -7 to 7
- norm_gain: float32 [4096], replicated, may hold values from 0.1 to 1.9
- curvature: bfloat16 [8, 512, 4096], P('fsdp'), may hold values from 0.19921875 to 2
- weight_slots: bfloat16 [4, 400, 128, 128], P('seq', 'fsdp'), may hold values from -1 to 1
- probe_slots: bfloat16 [4, 400, 128, 128], P('seq', 'fsdp'), may hold values from -0.09375 to 0.09375
- block_counts: int32 [4, 8], P('seq'), may hold values from 1 to 50, 320 in all within a row
Outputs:
- hvp_slots: float32 [4, 400, 128, 128], P('seq', 'fsdp')
The draws below stay inside these ranges and needn't reach their ends.
Inputs may be any that keep to these rules, and one draw needn't show every extreme that they name: `block_counts`: in each row, device d along fsdp owns the n_d blocks that follow the earlier devices' blocks, in its first n_d slots; a row sums to 320, and 50 is reached in every row.
All inputs are finite; a program needn't handle non-finite values.
Results may differ from the reference program's by a relative error of at most 0.018.
Values may be sent and summed in bfloat16 or wider, within the bound.
A program may use at most 128 MiB of HBM per device.

```python
import math
import jax
import jax.numpy as jnp
import numpy as np
from jax import lax

D = 4096
HQ = 16
HK = 4
HD = 128
BLK = 128
LEN = 512
NB = 320
SLOTS = 50
N_FSDP = 8
N_SEQ = 4


def draw_tokens(key, part):
    own_key = jax.random.fold_in(key, 11)
    noise = jax.random.normal(own_key, (N_FSDP, LEN, D), jnp.float32)
    result = jnp.clip(noise, -6.0, 6.0)
    return result.astype(jnp.bfloat16)


def draw_weight_slots(key, part):
    own_key = jax.random.fold_in(key, 12)
    result = jnp.clip(jax.random.normal(own_key, (N_SEQ, N_FSDP * SLOTS, BLK, BLK), jnp.float32), -6.0, 6.0) * D ** (-0.5)
    return result.astype(jnp.bfloat16)


def block_scale(key, extent, shards, least, largest):
    def one(axis_at, blocks):
        heights = jax.random.uniform(jax.random.fold_in(jax.random.fold_in(key, 6), axis_at), (blocks,), jnp.float32, least / len(shards), largest / len(shards))
        return jnp.repeat(jnp.exp(heights), extent[axis_at] // blocks).reshape((-1,) + (1,) * (len(extent) - axis_at - 1))

    gain = one(*shards[0])
    for cut in shards[1:]:
        gain = gain * one(*cut)
    return gain


def length_profile(number_of, total, reach, skew):
    weights = [(1 << 20) // math.isqrt(grade ** skew) + 1 for grade in range(2, number_of + 1)]
    surplus, holding = total - reach - (number_of - 1), [1] * (number_of - 1)
    while surplus > 0:
        candidates = [i for i in range(number_of - 1) if holding[i] < reach]
        whole, left = sum([weights[i] for i in candidates]), surplus
        for i in candidates:
            more = min(reach - holding[i], max(1, left * weights[i] // whole), surplus)
            holding[i] = holding[i] + more
            surplus = surplus - more
    return np.array([reach] + holding)


def ragged_sizes(key, count, total, bound, slope):
    if count == 2:
        one = jax.random.randint(key, (), max(1, total - bound), min(bound, total - 1) + 1)
        return jnp.stack([one, total - one])
    lengths = jnp.asarray(length_profile(count, total, bound, slope), jnp.int32)
    couples = (count - 1) // 2
    giver, receiver = lengths[1:1 + 2 * couples:2], lengths[2:2 + 2 * couples:2]
    margin = jnp.minimum(giver - 1, bound - receiver)
    moved = jax.random.randint(jax.random.fold_in(key, 1), (couples,), 0, 1 << 20) % (margin + 1)
    lengths = lengths.at[1:1 + 2 * couples:2].set(giver - moved).at[2:2 + 2 * couples:2].set(receiver + moved)
    return lengths[jax.random.permutation(jax.random.fold_in(key, 2), count)]


def centred(rng, dims, deviation, bound, cuts=(), kind=jnp.bfloat16):
    loudness = block_scale(rng, dims, cuts, -0.22, 0.18) if cuts else 1.0
    values = jax.random.normal(rng, dims, jnp.float32) * deviation * loudness
    return jnp.minimum(jnp.maximum(values, -bound), bound).astype(kind)


def setup_inputs(seed: int = 0) -> dict:
    streams_of = jax.random.split(jax.random.key(seed), 7)
    tokens = draw_tokens(jax.random.fold_in(streams_of[6], 71), 0)
    norm_gain = jnp.clip(1.0 + 0.18 * jax.random.normal(streams_of[1], (D,), jnp.float32), 0.1, 1.9)
    curvature = jnp.clip(jnp.exp(math.log(2.0) - 2.306499 * jax.random.uniform(streams_of[2], (N_FSDP, LEN, D), jnp.float32) ** block_scale(streams_of[2], (N_FSDP, LEN, D), ((0, 8),), -0.2, 0.2)), 0.19921875, 2.0).astype(jnp.bfloat16)
    weight_slots = draw_weight_slots(jax.random.fold_in(streams_of[6], 71), 0)
    probe_slots = centred(streams_of[4], (N_SEQ, N_FSDP * SLOTS, BLK, BLK), D ** -0.5, 0.09375, ((0, 4), (1, 8)))
    block_counts = jax.vmap(lambda own: ragged_sizes(own, N_FSDP, NB, SLOTS, 2))(jax.random.split(streams_of[5], N_SEQ)).reshape((N_SEQ, N_FSDP)).astype(jnp.int32)
    return dict(tokens=tokens, norm_gain=norm_gain, curvature=curvature, weight_slots=weight_slots, probe_slots=probe_slots, block_counts=block_counts)


THETA = 500000.0
EPS = 1e-05
NEGATIVE = -1e+30

def rotary(length, head_dim):
    half_dim = head_dim // 2
    frequency = jnp.exp(-jnp.log(THETA) * 2.0 * jnp.arange(half_dim, dtype=jnp.float32) / head_dim)
    angles = jnp.arange(length, dtype=jnp.float32)[:, None] * frequency[None, :]
    return (jnp.cos(angles)[:, None, :], jnp.sin(angles)[:, None, :])

def rotate(field_in, cosine, sine):
    half_dim = field_in.shape[-1] // 2
    first_half = field_in[..., :half_dim]
    second = field_in[..., half_dim:]
    return jnp.concatenate([first_half * cosine - second * sine, second * cosine + first_half * sine], axis=-1)

def normalize(tokens, norm_gain):
    values = tokens.astype(jnp.float32)
    factor = lax.rsqrt(lax.optimization_barrier(jnp.mean(values * values, axis=-1, keepdims=True)) + EPS)
    return (values * factor * norm_gain).astype(jnp.bfloat16)

def attention_branch(w_qkv, w_out, normed, cosine, sine, q_heads, kv_heads):
    length = normed.shape[0]
    head_dim = w_out.shape[0] // q_heads
    projected = jnp.dot(normed, w_qkv, preferred_element_type=jnp.float32)
    q_end = q_heads * head_dim
    k_end = q_end + kv_heads * head_dim
    queries = rotate(projected[:, :q_end].reshape(length, q_heads, head_dim), cosine, sine).astype(jnp.bfloat16)
    key_rows = rotate(projected[:, q_end:k_end].reshape(length, kv_heads, head_dim), cosine, sine).astype(jnp.bfloat16)
    values = projected[:, k_end:].reshape(length, kv_heads, head_dim).astype(jnp.bfloat16)
    queries, key_rows, values = lax.optimization_barrier((queries, key_rows, values))
    queries = queries.reshape(length, kv_heads, q_heads // kv_heads, head_dim)
    scores = jnp.einsum('qkgd,skd->kgqs', queries.astype(jnp.float32), key_rows.astype(jnp.float32)) * head_dim ** (-0.5)
    causal = jnp.arange(length)[:, None] >= jnp.arange(length)[None, :]
    scores = jnp.where(causal, scores, NEGATIVE)
    attn_probs = jax.nn.softmax(scores, axis=-1).astype(jnp.bfloat16)
    attn_probs = lax.optimization_barrier(attn_probs)
    mixed_heads = jnp.einsum('kgqs,skd->qkgd', attn_probs.astype(jnp.float32), values.astype(jnp.float32))
    mixed_heads = mixed_heads.reshape(length, q_heads * head_dim).astype(jnp.bfloat16)
    return jnp.dot(mixed_heads, w_out, preferred_element_type=jnp.float32)

def owner_slots(counts, blocks, slots):
    range_ends = jnp.cumsum(counts).astype(jnp.int32)
    starts = (range_ends - counts).astype(jnp.int32)
    block_ids = jnp.arange(blocks, dtype=jnp.int32)
    owners = lax.optimization_barrier(jnp.sum((range_ends[None, :] <= block_ids[:, None]).astype(jnp.int32), axis=1)).astype(jnp.int32)
    owner_hot = owners[:, None] == jnp.arange(counts.shape[0], dtype=jnp.int32)[None, :]
    first_block = lax.optimization_barrier(jnp.sum(jnp.where(owner_hot, starts[None, :], 0), axis=1)).astype(jnp.int32)
    return (owners * slots + block_ids - first_block).astype(jnp.int32)

def to_matrix(blocks, row_blocks, col_blocks):
    blk_edge = blocks.shape[-1]
    return blocks.reshape(row_blocks, col_blocks, blk_edge, blk_edge).transpose(0, 2, 1, 3).reshape(row_blocks * blk_edge, col_blocks * blk_edge)

def to_blocks(matrix, blk_edge):
    row_blocks = matrix.shape[0] // blk_edge
    col_blocks = matrix.shape[1] // blk_edge
    return matrix.reshape(row_blocks, blk_edge, col_blocks, blk_edge).transpose(0, 2, 1, 3).reshape(row_blocks * col_blocks, blk_edge, blk_edge)

def reference(tokens, norm_gain, curvature, weight_slots, probe_slots, block_counts):
    n_columns = weight_slots.shape[0]
    q_heads = HQ // n_columns
    kv_heads = HK // n_columns
    row_blocks = D // BLK
    qkv_cols = (q_heads + 2 * kv_heads) * HD // BLK
    out_rows = q_heads * HD // BLK
    qkv_split = row_blocks * qkv_cols
    cosine, sine = rotary(LEN, HD)
    normed = jax.vmap(normalize, in_axes=(0, None))(tokens, norm_gain)
    tangent_sum = jnp.zeros((N_FSDP, LEN, D), jnp.float32)
    unpacked = []
    for column in range(n_columns):
        slot_of = owner_slots(block_counts[column], NB, SLOTS)
        w_blocks = weight_slots[column][slot_of]
        p_blocks = probe_slots[column][slot_of]
        w_qkv = to_matrix(w_blocks[:qkv_split], row_blocks, qkv_cols)
        w_out = to_matrix(w_blocks[qkv_split:], out_rows, row_blocks)
        p_qkv = to_matrix(p_blocks[:qkv_split], row_blocks, qkv_cols)
        p_out = to_matrix(p_blocks[qkv_split:], out_rows, row_blocks)

        def tangent_one(seq_normed, w_qkv=w_qkv, w_out=w_out, p_qkv=p_qkv, p_out=p_out):

            def inner(first_w, second_w):
                return attention_branch(first_w, second_w, seq_normed, cosine, sine, q_heads, kv_heads)
            return jax.jvp(inner, (w_qkv, w_out), (p_qkv, p_out))[1]
        tangent_sum = tangent_sum + lax.map(tangent_one, normed)
        unpacked.append((slot_of, w_qkv, w_out))
    weighted = (curvature.astype(jnp.float32) * tangent_sum).astype(jnp.bfloat16)
    factor = 1.0 / jnp.sqrt(jnp.float32(LEN * N_FSDP))
    results = []
    for column in range(n_columns):
        slot_of, w_qkv, w_out = unpacked[column]

        def accumulate(grad_total, seq_pair, w_qkv=w_qkv, w_out=w_out):
            seq_normed, seq_weighted = seq_pair

            def inner(first_w, second_w):
                return attention_branch(first_w, second_w, seq_normed, cosine, sine, q_heads, kv_heads)
            _, pullback = jax.vjp(inner, w_qkv, w_out)
            g_qkv, g_out = pullback(seq_weighted.astype(jnp.float32))
            grad_blocks = jnp.concatenate([to_blocks(g_qkv, BLK), to_blocks(g_out, BLK)], axis=0)
            return (grad_total + grad_blocks.astype(jnp.float32), None)
        grad_total, _ = lax.scan(accumulate, jnp.zeros((NB, BLK, BLK), jnp.float32), (normed, weighted))
        packed = jnp.zeros((N_FSDP * SLOTS, BLK, BLK), jnp.float32).at[slot_of].set(grad_total * factor)
        results.append(packed)
    return jnp.stack(results)
```

```python
import functools

import jax
import jax.numpy as jnp
from jax import lax
from jax.experimental import pallas as pl
from jax.experimental.pallas import tpu as pltpu
from jax.sharding import PartitionSpec as P

D = 4096
HQ = 16
HK = 4
HD = 128
BLK = 128


THETA = 500000.0
EPS = 1e-05
NEGATIVE = -1e30


def rotary(length, head_dim):
    half_dim = head_dim // 2
    frequency = jnp.exp(-jnp.log(THETA) * 2.0 * jnp.arange(half_dim, dtype=jnp.float32) / head_dim)
    angles = jnp.arange(length, dtype=jnp.float32)[:, None] * frequency[None, :]
    return (jnp.cos(angles)[:, None, :], jnp.sin(angles)[:, None, :])


def rotate(field_in, cosine, sine):
    half_dim = field_in.shape[-1] // 2
    first_half = field_in[..., :half_dim]
    second = field_in[..., half_dim:]
    return jnp.concatenate(
        [first_half * cosine - second * sine, second * cosine + first_half * sine], axis=-1
    )


VMEM_BYTES = 62 * 1024 * 1024


def attention(projected, cosine, sine, q_heads, kv_heads):
    length = projected.shape[0]
    head_dim = projected.shape[1] // (q_heads + 2 * kv_heads)
    q_end = q_heads * head_dim
    k_end = q_end + kv_heads * head_dim
    queries = rotate(projected[:, :q_end].reshape(length, q_heads, head_dim), cosine, sine).astype(
        jnp.bfloat16
    )
    key_rows = rotate(
        projected[:, q_end:k_end].reshape(length, kv_heads, head_dim), cosine, sine
    ).astype(jnp.bfloat16)
    values = projected[:, k_end:].reshape(length, kv_heads, head_dim).astype(jnp.bfloat16)
    queries = queries.reshape(length, kv_heads, q_heads // kv_heads, head_dim)
    scores = jnp.einsum(
        "qkgd,skd->kgqs", queries, key_rows, preferred_element_type=jnp.float32
    ) * head_dim ** (-0.5)
    causal = jnp.arange(length)[:, None] >= jnp.arange(length)[None, :]
    scores = jnp.where(causal, scores, NEGATIVE)
    attn_probs = jax.nn.softmax(scores, axis=-1).astype(jnp.bfloat16)
    mixed_heads = jnp.einsum(
        "kgqs,skd->qkgd", attn_probs, values, preferred_element_type=jnp.float32
    )
    return mixed_heads.reshape(length, q_heads * head_dim).astype(jnp.bfloat16)


def ring_position(index, n):
    odd = lax.rem(index, 2)
    half = lax.div(index, 2)
    return (1 - odd) * half + odd * (n - 1 - half)


def ring_index(position, n):
    back = lax.div(position, n // 2)
    return (1 - back) * 2 * position + back * (2 * (n - 1 - position) + 1)


def pieces(slots):
    half = slots // 2
    out = []
    for direction, first, count in ((0, 0, half), (1, half, slots - half)):
        cuts = 5 if count % 5 == 0 else 1
        size = count // cuts
        out.append([(first + i * size, size) for i in range(cuts)])
    return out


def enter(neighbours):
    barrier = pltpu.get_barrier_semaphore()
    for neighbour in neighbours:
        pl.semaphore_signal(
            barrier, inc=1, device_id={"fsdp": neighbour}, device_id_type=pl.DeviceIdType.MESH
        )
    pl.semaphore_wait(barrier, len(neighbours))


def gather_kernel(n, slots, grid_qkv, grid_out, slot_ref, w_ref, p_ref, wq_ref, wo_ref, pq_ref,
                  po_ref, held_w, held_p, send_sem, recv_sem):
    me = lax.axis_index("fsdp")
    pos = ring_position(me, n)
    right = ring_index(lax.rem(pos + 1, n), n)
    left = ring_index(lax.rem(pos + n - 1, n), n)
    towards = (right, left)
    enter((left, right))
    parts = pieces(slots)
    arrays = ((w_ref, held_w), (p_ref, held_p))

    def copy(which, step, direction, j):
        own, held = arrays[which]
        first, size = parts[direction][j]
        shift = n - step if direction == 0 else step
        origin = ring_index(lax.rem(pos + shift, n), n)
        there = held.at[pl.ds(origin * slots + first, size)]
        here = own.at[pl.ds(first, size)] if step == 0 else there
        return pltpu.make_async_remote_copy(
            src_ref=here,
            dst_ref=there,
            send_sem=send_sem.at[which, step, direction, j],
            recv_sem=recv_sem.at[which, step, direction, j],
            device_id={"fsdp": towards[direction]},
            device_id_type=pl.DeviceIdType.MESH,
        )

    def arrival(which, step, direction, j):
        first, size = parts[direction][j]
        own, held = arrays[which]
        shift = n - step - 1 if direction == 0 else step + 1
        origin = ring_index(lax.rem(pos + shift, n), n)
        there = held.at[pl.ds(origin * slots + first, size)]
        pltpu.make_async_remote_copy(
            src_ref=there,
            dst_ref=there,
            send_sem=send_sem.at[which, step, direction, j],
            recv_sem=recv_sem.at[which, step, direction, j],
            device_id={"fsdp": towards[direction]},
            device_id_type=pl.DeviceIdType.MESH,
        ).wait_recv()

    def each():
        for j in range(max(len(parts[0]), len(parts[1]))):
            for direction in range(2):
                if j < len(parts[direction]):
                    yield direction, j

    def unpack(which, qkv_ref, out_ref):
        own, held = arrays[which]
        rows, cols = grid_qkv
        edge = held.shape[-1]

        def qkv_row(i, carry):
            for c in range(cols):
                qkv_ref[pl.ds(pl.multiple_of(i * edge, edge), edge), c * edge:(c + 1) * edge] = (
                    held[slot_ref[i * cols + c]]
                )
            return carry

        lax.fori_loop(0, rows, qkv_row, 0)
        out_rows, out_cols = grid_out

        def out_col(i, carry):
            for r in range(out_rows):
                out_ref[r * edge:(r + 1) * edge, pl.ds(pl.multiple_of(i * edge, edge), edge)] = (
                    held[slot_ref[rows * cols + r * out_cols + i]]
                )
            return carry

        lax.fori_loop(0, out_cols, out_col, 0)

    def finish(which, qkv_ref, out_ref):
        own, held = arrays[which]
        for direction, j in each():
            arrival(which, n - 2, direction, j)
        held[pl.ds(me * slots, slots)] = own[...]
        unpack(which, qkv_ref, out_ref)

    sent = []
    for which in range(2):
        for step in range(n - 1):
            for direction, j in each():
                if step > 0:
                    arrival(which, step - 1, direction, j)
                one = copy(which, step, direction, j)
                one.start()
                sent.append(one)
            if which == 1 and step == 0:
                finish(0, wq_ref, wo_ref)
    finish(1, pq_ref, po_ref)
    for one in sent:
        one.wait_send()


def gather_weights(slot_of, weights, probes, n, grid_qkv, grid_out):
    slots, edge, _ = weights.shape
    cuts = max(len(part) for part in pieces(slots))
    qkv = jax.ShapeDtypeStruct((grid_qkv[0] * edge, grid_qkv[1] * edge), jnp.bfloat16)
    out = jax.ShapeDtypeStruct((grid_out[0] * edge, grid_out[1] * edge), jnp.bfloat16)
    vmem = pl.BlockSpec(memory_space=pltpu.VMEM)
    return pl.pallas_call(
        functools.partial(gather_kernel, n, slots, grid_qkv, grid_out),
        out_shape=(qkv, out, qkv, out),
        in_specs=[pl.BlockSpec(memory_space=pltpu.SMEM), vmem, vmem],
        out_specs=(vmem,) * 4,
        scratch_shapes=[
            pltpu.VMEM((n * slots, edge, edge), jnp.bfloat16),
            pltpu.VMEM((n * slots, edge, edge), jnp.bfloat16),
            pltpu.SemaphoreType.DMA((2, n - 1, 2, cuts)),
            pltpu.SemaphoreType.DMA((2, n - 1, 2, cuts)),
        ],
        compiler_params=pltpu.CompilerParams(
            collective_id=0, has_side_effects=True, vmem_limit_bytes=VMEM_BYTES
        ),
    )(slot_of, weights, probes)


def gradient_kernel(grid_qkv, grid_out, slot_ref, normed_ref, d_proj_ref, mixed_t_ref,
                    weighted_ref, out_ref):
    edge = out_ref.shape[-1]
    rows, cols = grid_qkv
    out_rows, out_cols = grid_out
    group = 2

    def clear(i, carry):
        out_ref[i] = jnp.zeros(out_ref.shape[1:], out_ref.dtype)
        return carry

    lax.fori_loop(0, out_ref.shape[0], clear, 0)

    def qkv_rows(i, carry):
        width = group * edge
        left = normed_ref[:, pl.ds(pl.multiple_of(i * width, width), width)]
        block = lax.dot_general(
            left, d_proj_ref[...], (((0,), (0,)), ((), ())), preferred_element_type=jnp.float32
        ).astype(jnp.bfloat16)
        for r in range(group):
            for c in range(cols):
                out_ref[slot_ref[(i * group + r) * cols + c]] = block[
                    r * edge:(r + 1) * edge, c * edge:(c + 1) * edge
                ]
        return carry

    lax.fori_loop(0, rows // group, qkv_rows, 0)

    def out_columns(i, carry):
        width = group * edge
        right = weighted_ref[:, pl.ds(pl.multiple_of(i * width, width), width)]
        block = jnp.dot(
            mixed_t_ref[...], right, preferred_element_type=jnp.float32
        ).astype(jnp.bfloat16)
        for r in range(out_rows):
            for c in range(group):
                out_ref[slot_ref[rows * cols + r * out_cols + i * group + c]] = block[
                    r * edge:(r + 1) * edge, c * edge:(c + 1) * edge
                ]
        return carry

    lax.fori_loop(0, out_cols // group, out_columns, 0)


def gradient_slots(slot_of, normed, d_proj, mixed_t, weighted, total_slots, grid_qkv, grid_out):
    vmem = pl.BlockSpec(memory_space=pltpu.VMEM)
    return pl.pallas_call(
        functools.partial(gradient_kernel, grid_qkv, grid_out),
        out_shape=jax.ShapeDtypeStruct((total_slots, BLK, BLK), jnp.bfloat16),
        in_specs=[pl.BlockSpec(memory_space=pltpu.SMEM)] + [vmem] * 4,
        out_specs=vmem,
        compiler_params=pltpu.CompilerParams(vmem_limit_bytes=VMEM_BYTES),
    )(slot_of, normed, d_proj, mixed_t, weighted)


def reduce_kernel(n, slots, scale, g_ref, out_ref, held, send_sem, recv_sem):
    me = lax.axis_index("fsdp")
    pos = ring_position(me, n)
    right = ring_index(lax.rem(pos + 1, n), n)
    left = ring_index(lax.rem(pos + n - 1, n), n)
    towards = (right, left)
    enter((left, right))
    parts = pieces(slots)

    def own(step, direction, j):
        first, size = parts[direction][j]
        shift = n - 1 - step if direction == 0 else 1 + step
        target = ring_index(lax.rem(pos + shift, n), n)
        return pl.ds(target * slots + first, size)

    def copy(step, direction, j):
        first, size = parts[direction][j]
        here = g_ref.at[own(0, direction, j)] if step == 0 else held.at[step - 1, pl.ds(first, size)]
        return pltpu.make_async_remote_copy(
            src_ref=here,
            dst_ref=held.at[step, pl.ds(first, size)],
            send_sem=send_sem.at[step, direction, j],
            recv_sem=recv_sem.at[step, direction, j],
            device_id={"fsdp": towards[direction]},
            device_id_type=pl.DeviceIdType.MESH,
        )

    def each():
        for j in range(max(len(parts[0]), len(parts[1]))):
            for direction in range(2):
                if j < len(parts[direction]):
                    yield direction, j

    sent = {}
    for step in range(n - 1):
        for direction, j in each():
            first, size = parts[direction][j]
            if step > 0:
                sent[step - 1, direction, j].wait_recv()
                held[step - 1, pl.ds(first, size)] = (
                    held[step - 1, pl.ds(first, size)].astype(jnp.float32)
                    + g_ref[own(step, direction, j)].astype(jnp.float32)
                ).astype(jnp.bfloat16)
            one = copy(step, direction, j)
            one.start()
            sent[step, direction, j] = one
    for direction, j in each():
        first, size = parts[direction][j]
        sent[n - 2, direction, j].wait_recv()
        out_ref[pl.ds(first, size)] = (
            held[n - 2, pl.ds(first, size)].astype(jnp.float32)
            + g_ref[own(n - 1, direction, j)].astype(jnp.float32)
        ) * scale
    for one in sent.values():
        one.wait_send()


def reduce_slots(partial_slots, n, scale):
    total, edge, _ = partial_slots.shape
    slots = total // n
    cuts = max(len(part) for part in pieces(slots))
    vmem = pl.BlockSpec(memory_space=pltpu.VMEM)
    return pl.pallas_call(
        functools.partial(reduce_kernel, n, slots, scale),
        out_shape=jax.ShapeDtypeStruct((slots, edge, edge), jnp.float32),
        in_specs=[vmem],
        out_specs=vmem,
        scratch_shapes=[
            pltpu.VMEM((n - 1, slots, edge, edge), jnp.bfloat16),
            pltpu.SemaphoreType.DMA((n - 1, 2, cuts)),
            pltpu.SemaphoreType.DMA((n - 1, 2, cuts)),
        ],
        compiler_params=pltpu.CompilerParams(
            collective_id=1, has_side_effects=True, vmem_limit_bytes=VMEM_BYTES
        ),
    )(partial_slots)


def local(tokens, norm_gain, curvature, weight_slots, probe_slots, block_counts):
    n_columns = lax.axis_size("seq")
    n_owners = lax.axis_size("fsdp")
    q_heads = HQ // n_columns
    kv_heads = HK // n_columns
    row_blocks = D // BLK
    qkv_cols = (q_heads + 2 * kv_heads) * HD // BLK
    out_rows = q_heads * HD // BLK
    grid_qkv, grid_out = (row_blocks, qkv_cols), (out_rows, row_blocks)
    total_blocks = row_blocks * qkv_cols + out_rows * row_blocks
    slots = weight_slots.shape[1]
    length = tokens.shape[1]
    counts = block_counts[0]
    range_ends = jnp.cumsum(counts)
    starts = range_ends - counts
    owner_ids = jnp.arange(n_owners, dtype=jnp.int32)
    block_ids = jnp.arange(total_blocks, dtype=jnp.int32)
    owners = jnp.sum((range_ends[None, :] <= block_ids[:, None]).astype(jnp.int32), axis=1)
    first_block = jnp.sum(
        jnp.where(owners[:, None] == owner_ids[None, :], starts[None, :], 0), axis=1
    )
    slot_of = (owners * slots + block_ids - first_block).astype(jnp.int32)
    w_qkv, w_out, p_qkv, p_out = gather_weights(
        slot_of, weight_slots[0], probe_slots[0], n_owners, grid_qkv, grid_out
    )
    values = tokens[0].astype(jnp.float32)
    factor = lax.rsqrt(jnp.mean(values * values, axis=-1, keepdims=True) + EPS)
    normed = (values * factor * norm_gain).astype(jnp.bfloat16)
    cosine, sine = rotary(length, HD)

    def inner(projected):
        return attention(projected, cosine, sine, q_heads, kv_heads)

    projected = jnp.dot(normed, w_qkv, preferred_element_type=jnp.float32)
    d_projected = jnp.dot(normed, p_qkv, preferred_element_type=jnp.float32)
    mixed, d_mixed = jax.jvp(inner, (projected,), (d_projected,))
    tangent = jnp.dot(d_mixed, w_out, preferred_element_type=jnp.float32) + jnp.dot(
        mixed, p_out, preferred_element_type=jnp.float32
    )
    share = lax.psum_scatter(
        tangent.astype(jnp.bfloat16), "seq", scatter_dimension=1, tiled=True
    ).astype(jnp.float32)
    share_width = share.shape[1]
    curv_share = lax.dynamic_slice_in_dim(
        curvature[0], lax.axis_index("seq") * share_width, share_width, 1
    )
    weighted_share = (curv_share.astype(jnp.float32) * share).astype(jnp.bfloat16)
    weighted = lax.all_gather(weighted_share, "seq", axis=1, tiled=True)
    mixed_again, pullback = jax.vjp(inner, projected)
    back_mixed = lax.dot_general(
        weighted, w_out, (((1,), (1,)), ((), ())), preferred_element_type=jnp.float32
    ).astype(jnp.bfloat16)
    (back_projected,) = pullback(back_mixed)
    partial_slots = gradient_slots(
        slot_of,
        normed,
        back_projected.astype(jnp.bfloat16),
        mixed_again.T,
        weighted,
        n_owners * slots,
        grid_qkv,
        grid_out,
    )
    scaled = reduce_slots(partial_slots, n_owners, (length * n_owners) ** -0.5)
    return scaled.reshape(1, slots, BLK, BLK)


def solution(mesh):
    in_specs = (
        P("fsdp", None, None),
        P(),
        P("fsdp", None, None),
        P("seq", "fsdp", None, None),
        P("seq", "fsdp", None, None),
        P("seq", None),
    )
    out_specs = P("seq", "fsdp", None, None)
    return jax.shard_map(local, mesh=mesh, in_specs=in_specs, out_specs=out_specs, check_vma=False)
```

```python
import functools

import jax
import jax.numpy as jnp
from jax import lax
from jax.experimental import pallas as pl
from jax.experimental.pallas import tpu as pltpu
from jax.sharding import PartitionSpec as P

D = 4096
HQ = 16
HK = 4
HD = 128
BLK = 128


THETA = 500000.0
EPS = 1e-05
NEGATIVE = -1e30


def rotary(length, head_dim):
    half_dim = head_dim // 2
    frequency = jnp.exp(-jnp.log(THETA) * 2.0 * jnp.arange(half_dim, dtype=jnp.float32) / head_dim)
    angles = jnp.arange(length, dtype=jnp.float32)[:, None] * frequency[None, :]
    return (jnp.cos(angles)[:, None, :], jnp.sin(angles)[:, None, :])


def rotate(field_in, cosine, sine):
    half_dim = field_in.shape[-1] // 2
    first_half = field_in[..., :half_dim]
    second = field_in[..., half_dim:]
    return jnp.concatenate(
        [first_half * cosine - second * sine, second * cosine + first_half * sine], axis=-1
    )


VMEM_BYTES = 62 * 1024 * 1024


def attention(projected, cosine, sine, q_heads, kv_heads):
    length = projected.shape[0]
    head_dim = projected.shape[1] // (q_heads + 2 * kv_heads)
    q_end = q_heads * head_dim
    k_end = q_end + kv_heads * head_dim
    queries = rotate(projected[:, :q_end].reshape(length, q_heads, head_dim), cosine, sine).astype(
        jnp.bfloat16
    )
    key_rows = rotate(
        projected[:, q_end:k_end].reshape(length, kv_heads, head_dim), cosine, sine
    ).astype(jnp.bfloat16)
    values = projected[:, k_end:].reshape(length, kv_heads, head_dim).astype(jnp.bfloat16)
    queries = queries.reshape(length, kv_heads, q_heads // kv_heads, head_dim)
    scores = jnp.einsum(
        "qkgd,skd->kgqs", queries, key_rows, preferred_element_type=jnp.float32
    ) * head_dim ** (-0.5)
    causal = jnp.arange(length)[:, None] >= jnp.arange(length)[None, :]
    scores = jnp.where(causal, scores, NEGATIVE)
    attn_probs = jax.nn.softmax(scores, axis=-1).astype(jnp.bfloat16)
    mixed_heads = jnp.einsum(
        "kgqs,skd->qkgd", attn_probs, values, preferred_element_type=jnp.float32
    )
    return mixed_heads.reshape(length, q_heads * head_dim).astype(jnp.bfloat16)


def ring_position(index, n):
    odd = lax.rem(index, 2)
    half = lax.div(index, 2)
    return (1 - odd) * half + odd * (n - 1 - half)


def ring_index(position, n):
    back = lax.div(position, n // 2)
    return (1 - back) * 2 * position + back * (2 * (n - 1 - position) + 1)


def pieces(slots):
    half = slots // 2
    out = []
    for direction, first, count in ((0, 0, half), (1, half, slots - half)):
        cuts = 5 if count % 5 == 0 else 1
        size = count // cuts
        out.append([(first + i * size, size) for i in range(cuts)])
    return out


def enter(neighbours, axis="fsdp"):
    barrier = pltpu.get_barrier_semaphore()
    for neighbour in neighbours:
        pl.semaphore_signal(
            barrier, inc=1, device_id={axis: neighbour}, device_id_type=pl.DeviceIdType.MESH
        )
    pl.semaphore_wait(barrier, len(neighbours))


def gather_kernel(n, slots, grid_qkv, grid_out, slot_ref, w_ref, p_ref, wq_ref, wo_ref, pq_ref,
                  po_ref, held_w, held_p, send_sem, recv_sem):
    me = lax.axis_index("fsdp")
    pos = ring_position(me, n)
    right = ring_index(lax.rem(pos + 1, n), n)
    left = ring_index(lax.rem(pos + n - 1, n), n)
    towards = (right, left)
    enter((left, right))
    parts = pieces(slots)
    arrays = ((w_ref, held_w), (p_ref, held_p))

    def copy(which, step, direction, j):
        own, held = arrays[which]
        first, size = parts[direction][j]
        shift = n - step if direction == 0 else step
        origin = ring_index(lax.rem(pos + shift, n), n)
        there = held.at[pl.ds(origin * slots + first, size)]
        here = own.at[pl.ds(first, size)] if step == 0 else there
        return pltpu.make_async_remote_copy(
            src_ref=here,
            dst_ref=there,
            send_sem=send_sem.at[which, step, direction, j],
            recv_sem=recv_sem.at[which, step, direction, j],
            device_id={"fsdp": towards[direction]},
            device_id_type=pl.DeviceIdType.MESH,
        )

    def arrival(which, step, direction, j):
        first, size = parts[direction][j]
        own, held = arrays[which]
        shift = n - step - 1 if direction == 0 else step + 1
        origin = ring_index(lax.rem(pos + shift, n), n)
        there = held.at[pl.ds(origin * slots + first, size)]
        pltpu.make_async_remote_copy(
            src_ref=there,
            dst_ref=there,
            send_sem=send_sem.at[which, step, direction, j],
            recv_sem=recv_sem.at[which, step, direction, j],
            device_id={"fsdp": towards[direction]},
            device_id_type=pl.DeviceIdType.MESH,
        ).wait_recv()

    def each():
        for j in range(max(len(parts[0]), len(parts[1]))):
            for direction in range(2):
                if j < len(parts[direction]):
                    yield direction, j

    def unpack(which, qkv_ref, out_ref):
        own, held = arrays[which]
        rows, cols = grid_qkv
        edge = held.shape[-1]

        def qkv_row(i, carry):
            for c in range(cols):
                qkv_ref[pl.ds(pl.multiple_of(i * edge, edge), edge), c * edge:(c + 1) * edge] = (
                    held[slot_ref[i * cols + c]]
                )
            return carry

        lax.fori_loop(0, rows, qkv_row, 0)
        out_rows, out_cols = grid_out

        def out_col(i, carry):
            for r in range(out_rows):
                out_ref[r * edge:(r + 1) * edge, pl.ds(pl.multiple_of(i * edge, edge), edge)] = (
                    held[slot_ref[rows * cols + r * out_cols + i]]
                )
            return carry

        lax.fori_loop(0, out_cols, out_col, 0)

    def finish(which, qkv_ref, out_ref):
        own, held = arrays[which]
        for direction, j in each():
            arrival(which, n - 2, direction, j)
        held[pl.ds(me * slots, slots)] = own[...]
        unpack(which, qkv_ref, out_ref)

    sent = []
    for which in range(2):
        for step in range(n - 1):
            for direction, j in each():
                if step > 0:
                    arrival(which, step - 1, direction, j)
                one = copy(which, step, direction, j)
                one.start()
                sent.append(one)
            if which == 1 and step == 0:
                finish(0, wq_ref, wo_ref)
    finish(1, pq_ref, po_ref)
    for one in sent:
        one.wait_send()


def gather_weights(slot_of, weights, probes, n, grid_qkv, grid_out):
    slots, edge, _ = weights.shape
    cuts = max(len(part) for part in pieces(slots))
    qkv = jax.ShapeDtypeStruct((grid_qkv[0] * edge, grid_qkv[1] * edge), jnp.bfloat16)
    out = jax.ShapeDtypeStruct((grid_out[0] * edge, grid_out[1] * edge), jnp.bfloat16)
    vmem = pl.BlockSpec(memory_space=pltpu.VMEM)
    return pl.pallas_call(
        functools.partial(gather_kernel, n, slots, grid_qkv, grid_out),
        out_shape=(qkv, out, qkv, out),
        in_specs=[pl.BlockSpec(memory_space=pltpu.SMEM), vmem, vmem],
        out_specs=(vmem,) * 4,
        scratch_shapes=[
            pltpu.VMEM((n * slots, edge, edge), jnp.bfloat16),
            pltpu.VMEM((n * slots, edge, edge), jnp.bfloat16),
            pltpu.SemaphoreType.DMA((2, n - 1, 2, cuts)),
            pltpu.SemaphoreType.DMA((2, n - 1, 2, cuts)),
        ],
        compiler_params=pltpu.CompilerParams(
            collective_id=0, has_side_effects=True, vmem_limit_bytes=VMEM_BYTES
        ),
    )(slot_of, weights, probes)


def gradient_kernel(grid_qkv, grid_out, slot_ref, normed_ref, d_proj_ref, mixed_t_ref,
                    weighted_ref, out_ref):
    edge = out_ref.shape[-1]
    rows, cols = grid_qkv
    out_rows, out_cols = grid_out
    group = 2

    def clear(i, carry):
        out_ref[i] = jnp.zeros(out_ref.shape[1:], out_ref.dtype)
        return carry

    lax.fori_loop(0, out_ref.shape[0], clear, 0)

    def qkv_rows(i, carry):
        width = group * edge
        left = normed_ref[:, pl.ds(pl.multiple_of(i * width, width), width)]
        block = lax.dot_general(
            left, d_proj_ref[...], (((0,), (0,)), ((), ())), preferred_element_type=jnp.float32
        ).astype(jnp.bfloat16)
        for r in range(group):
            for c in range(cols):
                out_ref[slot_ref[(i * group + r) * cols + c]] = block[
                    r * edge:(r + 1) * edge, c * edge:(c + 1) * edge
                ]
        return carry

    lax.fori_loop(0, rows // group, qkv_rows, 0)

    def out_columns(i, carry):
        width = group * edge
        right = weighted_ref[:, pl.ds(pl.multiple_of(i * width, width), width)]
        block = jnp.dot(
            mixed_t_ref[...], right, preferred_element_type=jnp.float32
        ).astype(jnp.bfloat16)
        for r in range(out_rows):
            for c in range(group):
                out_ref[slot_ref[rows * cols + r * out_cols + i * group + c]] = block[
                    r * edge:(r + 1) * edge, c * edge:(c + 1) * edge
                ]
        return carry

    lax.fori_loop(0, out_cols // group, out_columns, 0)


def gradient_slots(slot_of, normed, d_proj, mixed_t, weighted, total_slots, grid_qkv, grid_out):
    vmem = pl.BlockSpec(memory_space=pltpu.VMEM)
    return pl.pallas_call(
        functools.partial(gradient_kernel, grid_qkv, grid_out),
        out_shape=jax.ShapeDtypeStruct((total_slots, BLK, BLK), jnp.bfloat16),
        in_specs=[pl.BlockSpec(memory_space=pltpu.SMEM)] + [vmem] * 4,
        out_specs=vmem,
        compiler_params=pltpu.CompilerParams(vmem_limit_bytes=VMEM_BYTES),
    )(slot_of, normed, d_proj, mixed_t, weighted)


def reduce_kernel(n, slots, scale, g_ref, out_ref, held, send_sem, recv_sem):
    me = lax.axis_index("fsdp")
    pos = ring_position(me, n)
    right = ring_index(lax.rem(pos + 1, n), n)
    left = ring_index(lax.rem(pos + n - 1, n), n)
    towards = (right, left)
    enter((left, right))
    parts = pieces(slots)

    def own(step, direction, j):
        first, size = parts[direction][j]
        shift = n - 1 - step if direction == 0 else 1 + step
        target = ring_index(lax.rem(pos + shift, n), n)
        return pl.ds(target * slots + first, size)

    def copy(step, direction, j):
        first, size = parts[direction][j]
        here = g_ref.at[own(0, direction, j)] if step == 0 else held.at[step - 1, pl.ds(first, size)]
        return pltpu.make_async_remote_copy(
            src_ref=here,
            dst_ref=held.at[step, pl.ds(first, size)],
            send_sem=send_sem.at[step, direction, j],
            recv_sem=recv_sem.at[step, direction, j],
            device_id={"fsdp": towards[direction]},
            device_id_type=pl.DeviceIdType.MESH,
        )

    def each():
        for j in range(max(len(parts[0]), len(parts[1]))):
            for direction in range(2):
                if j < len(parts[direction]):
                    yield direction, j

    sent = {}
    for step in range(n - 1):
        for direction, j in each():
            first, size = parts[direction][j]
            if step > 0:
                sent[step - 1, direction, j].wait_recv()
                held[step - 1, pl.ds(first, size)] = (
                    held[step - 1, pl.ds(first, size)].astype(jnp.float32)
                    + g_ref[own(step, direction, j)].astype(jnp.float32)
                ).astype(jnp.bfloat16)
            one = copy(step, direction, j)
            one.start()
            sent[step, direction, j] = one
    for direction, j in each():
        first, size = parts[direction][j]
        sent[n - 2, direction, j].wait_recv()
        out_ref[pl.ds(first, size)] = (
            held[n - 2, pl.ds(first, size)].astype(jnp.float32)
            + g_ref[own(n - 1, direction, j)].astype(jnp.float32)
        ) * scale
    for one in sent.values():
        one.wait_send()


def reduce_slots(partial_slots, n, scale):
    total, edge, _ = partial_slots.shape
    slots = total // n
    cuts = max(len(part) for part in pieces(slots))
    vmem = pl.BlockSpec(memory_space=pltpu.VMEM)
    return pl.pallas_call(
        functools.partial(reduce_kernel, n, slots, scale),
        out_shape=jax.ShapeDtypeStruct((slots, edge, edge), jnp.float32),
        in_specs=[vmem],
        out_specs=vmem,
        scratch_shapes=[
            pltpu.VMEM((n - 1, slots, edge, edge), jnp.bfloat16),
            pltpu.SemaphoreType.DMA((n - 1, 2, cuts)),
            pltpu.SemaphoreType.DMA((n - 1, 2, cuts)),
        ],
        compiler_params=pltpu.CompilerParams(
            collective_id=1, has_side_effects=True, vmem_limit_bytes=VMEM_BYTES
        ),
    )(partial_slots)


def exchange_kernel(mixed_ref, d_mixed_ref, w_ref, p_ref, curv_ref, weighted_ref, back_ref,
                    terms, near, pair, far, share, rest, send_sem, recv_sem):
    me = lax.axis_index("seq")
    side = lax.rem(me, 2)
    core = me + 1 - 2 * side
    across = me + 2 - 4 * lax.rem(lax.div(me, 2), 2)
    enter((core, across), "seq")
    length, width = terms.shape
    half = width // 2
    chunks = recv_sem.shape[1]
    rows = length // chunks
    mine = pl.ds(pl.multiple_of(side * half, half), half)
    other = pl.ds(pl.multiple_of((1 - side) * half, half), half)

    def block(i):
        return pl.ds(i * rows, rows)

    def copy(stage, i, here, there, target):
        return pltpu.make_async_remote_copy(
            src_ref=here,
            dst_ref=there,
            send_sem=send_sem.at[stage, i],
            recv_sem=recv_sem.at[stage, i],
            device_id={"seq": target},
            device_id_type=pl.DeviceIdType.MESH,
        )

    def terms_of(i):
        tile = width // 4

        def columns(j, carry):
            cols = pl.ds(pl.multiple_of(j * tile, tile), tile)
            terms[block(i), cols] = (
                jnp.dot(d_mixed_ref[block(i), :], w_ref[:, cols], preferred_element_type=jnp.float32)
                + jnp.dot(mixed_ref[block(i), :], p_ref[:, cols], preferred_element_type=jnp.float32)
            ).astype(jnp.bfloat16)
            return carry

        lax.fori_loop(0, 4, columns, 0)

    first = [copy(0, i, terms.at[block(i), other], near.at[block(i)], core) for i in range(chunks)]
    second = [copy(1, i, pair.at[block(i)], far.at[block(i)], across) for i in range(chunks)]
    third = [copy(2, i, share.at[block(i)], rest.at[block(i)], core) for i in range(chunks)]

    def send_pair(i):
        first[i].wait_recv()
        pair[block(i)] = (
            terms[block(i), mine].astype(jnp.float32) + near[block(i)].astype(jnp.float32)
        ).astype(jnp.bfloat16)
        second[i].start()

    def send_share(i):
        second[i].wait_recv()
        total = pair[block(i)].astype(jnp.float32) + far[block(i)].astype(jnp.float32)
        share[block(i)] = (curv_ref[block(i), mine].astype(jnp.float32) * total).astype(
            jnp.bfloat16
        )
        third[i].start()

    def finish(i):
        weighted_ref[block(i), mine] = share[block(i)]
        third[i].wait_recv()
        weighted_ref[block(i), other] = rest[block(i)]
        back_ref[block(i), :] = lax.dot_general(
            weighted_ref[block(i), :],
            w_ref[...],
            (((1,), (1,)), ((), ())),
            preferred_element_type=jnp.float32,
        ).astype(jnp.bfloat16)

    for i in range(chunks):
        terms_of(i)
        first[i].start()
        if i > 0:
            send_pair(i - 1)
    send_pair(chunks - 1)
    for i in range(chunks):
        send_share(i)
        if i > 0:
            finish(i - 1)
    finish(chunks - 1)
    for one in first + second + third:
        one.wait_send()


def exchange(mixed, d_mixed, w_out, p_out, curvature):
    length, width = curvature.shape
    chunks = 4
    vmem = pl.BlockSpec(memory_space=pltpu.VMEM)
    half = pltpu.VMEM((length, width // 2), jnp.bfloat16)
    return pl.pallas_call(
        exchange_kernel,
        out_shape=(
            jax.ShapeDtypeStruct((length, width), jnp.bfloat16),
            jax.ShapeDtypeStruct(mixed.shape, jnp.bfloat16),
        ),
        in_specs=[vmem] * 5,
        out_specs=(vmem, vmem),
        scratch_shapes=[
            pltpu.VMEM((length, width), jnp.bfloat16),
            half,
            half,
            half,
            half,
            half,
            pltpu.SemaphoreType.DMA((3, chunks)),
            pltpu.SemaphoreType.DMA((3, chunks)),
        ],
        compiler_params=pltpu.CompilerParams(
            collective_id=2, has_side_effects=True, vmem_limit_bytes=VMEM_BYTES
        ),
    )(mixed, d_mixed, w_out, p_out, curvature)


def local(tokens, norm_gain, curvature, weight_slots, probe_slots, block_counts):
    n_columns = lax.axis_size("seq")
    n_owners = lax.axis_size("fsdp")
    q_heads = HQ // n_columns
    kv_heads = HK // n_columns
    row_blocks = D // BLK
    qkv_cols = (q_heads + 2 * kv_heads) * HD // BLK
    out_rows = q_heads * HD // BLK
    grid_qkv, grid_out = (row_blocks, qkv_cols), (out_rows, row_blocks)
    total_blocks = row_blocks * qkv_cols + out_rows * row_blocks
    slots = weight_slots.shape[1]
    length = tokens.shape[1]
    counts = block_counts[0]
    range_ends = jnp.cumsum(counts)
    starts = range_ends - counts
    owner_ids = jnp.arange(n_owners, dtype=jnp.int32)
    block_ids = jnp.arange(total_blocks, dtype=jnp.int32)
    owners = jnp.sum((range_ends[None, :] <= block_ids[:, None]).astype(jnp.int32), axis=1)
    first_block = jnp.sum(
        jnp.where(owners[:, None] == owner_ids[None, :], starts[None, :], 0), axis=1
    )
    slot_of = (owners * slots + block_ids - first_block).astype(jnp.int32)
    w_qkv, w_out, p_qkv, p_out = gather_weights(
        slot_of, weight_slots[0], probe_slots[0], n_owners, grid_qkv, grid_out
    )
    values = tokens[0].astype(jnp.float32)
    factor = lax.rsqrt(jnp.mean(values * values, axis=-1, keepdims=True) + EPS)
    normed = (values * factor * norm_gain).astype(jnp.bfloat16)
    cosine, sine = rotary(length, HD)

    def inner(projected):
        return attention(projected, cosine, sine, q_heads, kv_heads)

    projected = jnp.dot(normed, w_qkv, preferred_element_type=jnp.float32)
    d_projected = jnp.dot(normed, p_qkv, preferred_element_type=jnp.float32)
    mixed, d_mixed = jax.jvp(inner, (projected,), (d_projected,))
    weighted, back_mixed = exchange(mixed, d_mixed, w_out, p_out, curvature[0])
    mixed_again, pullback = jax.vjp(inner, projected)
    (back_projected,) = pullback(back_mixed)
    partial_slots = gradient_slots(
        slot_of,
        normed,
        back_projected.astype(jnp.bfloat16),
        mixed_again.T,
        weighted,
        n_owners * slots,
        grid_qkv,
        grid_out,
    )
    scaled = reduce_slots(partial_slots, n_owners, (length * n_owners) ** -0.5)
    return scaled.reshape(1, slots, BLK, BLK)


def solution(mesh):
    in_specs = (
        P("fsdp", None, None),
        P(),
        P("fsdp", None, None),
        P("seq", "fsdp", None, None),
        P("seq", "fsdp", None, None),
        P("seq", None),
    )
    out_specs = P("seq", "fsdp", None, None)
    return jax.shard_map(local, mesh=mesh, in_specs=in_specs, out_specs=out_specs, check_vma=False)
```

```python
import functools

import jax
import jax.numpy as jnp
from jax import lax
from jax.experimental import pallas as pl
from jax.experimental.pallas import tpu as pltpu
from jax.sharding import PartitionSpec as P

D = 4096
HQ = 16
HK = 4
HD = 128
BLK = 128


THETA = 500000.0
EPS = 1e-05
NEGATIVE = -1e30


def rotary(length, head_dim):
    half_dim = head_dim // 2
    frequency = jnp.exp(-jnp.log(THETA) * 2.0 * jnp.arange(half_dim, dtype=jnp.float32) / head_dim)
    angles = jnp.arange(length, dtype=jnp.float32)[:, None] * frequency[None, :]
    return (jnp.cos(angles)[:, None, :], jnp.sin(angles)[:, None, :])


def rotate(field_in, cosine, sine):
    half_dim = field_in.shape[-1] // 2
    first_half = field_in[..., :half_dim]
    second = field_in[..., half_dim:]
    return jnp.concatenate(
        [first_half * cosine - second * sine, second * cosine + first_half * sine], axis=-1
    )


VMEM_BYTES = 62 * 1024 * 1024


def attention(projected, cosine, sine, q_heads, kv_heads):
    length = projected.shape[0]
    head_dim = projected.shape[1] // (q_heads + 2 * kv_heads)
    q_end = q_heads * head_dim
    k_end = q_end + kv_heads * head_dim
    queries = rotate(projected[:, :q_end].reshape(length, q_heads, head_dim), cosine, sine).astype(
        jnp.bfloat16
    )
    key_rows = rotate(
        projected[:, q_end:k_end].reshape(length, kv_heads, head_dim), cosine, sine
    ).astype(jnp.bfloat16)
    values = projected[:, k_end:].reshape(length, kv_heads, head_dim).astype(jnp.bfloat16)
    queries = queries.reshape(length, kv_heads, q_heads // kv_heads, head_dim)
    scores = jnp.einsum(
        "qkgd,skd->kgqs", queries, key_rows, preferred_element_type=jnp.float32
    ) * head_dim ** (-0.5)
    causal = jnp.arange(length)[:, None] >= jnp.arange(length)[None, :]
    scores = jnp.where(causal, scores, NEGATIVE)
    attn_probs = jax.nn.softmax(scores, axis=-1).astype(jnp.bfloat16)
    mixed_heads = jnp.einsum(
        "kgqs,skd->qkgd", attn_probs, values, preferred_element_type=jnp.float32
    )
    return mixed_heads.reshape(length, q_heads * head_dim).astype(jnp.bfloat16)


def ring_position(index, n):
    odd = lax.rem(index, 2)
    half = lax.div(index, 2)
    return (1 - odd) * half + odd * (n - 1 - half)


def ring_index(position, n):
    back = lax.div(position, n // 2)
    return (1 - back) * 2 * position + back * (2 * (n - 1 - position) + 1)


def pieces(slots):
    half = slots // 2
    out = []
    for direction, first, count in ((0, 0, half), (1, half, slots - half)):
        cuts = 5 if count % 5 == 0 else 1
        size = count // cuts
        out.append([(first + i * size, size) for i in range(cuts)])
    return out


def enter(neighbours, axis="fsdp"):
    barrier = pltpu.get_barrier_semaphore()
    for neighbour in neighbours:
        pl.semaphore_signal(
            barrier, inc=1, device_id={axis: neighbour}, device_id_type=pl.DeviceIdType.MESH
        )
    pl.semaphore_wait(barrier, len(neighbours))


def gather_kernel(n, slots, grid_qkv, grid_out, slot_ref, w_ref, p_ref, tokens_ref, gain_ref,
                  proj_ref, d_proj_ref, wo_ref, po_ref, normed_t_ref, held_w, held_p, matrix,
                  normed, send_sem, recv_sem):
    me = lax.axis_index("fsdp")
    pos = ring_position(me, n)
    right = ring_index(lax.rem(pos + 1, n), n)
    left = ring_index(lax.rem(pos + n - 1, n), n)
    towards = (right, left)
    enter((left, right))
    parts = pieces(slots)
    arrays = ((w_ref, held_w), (p_ref, held_p))

    def copy(which, step, direction, j):
        own, held = arrays[which]
        first, size = parts[direction][j]
        shift = n - step if direction == 0 else step
        origin = ring_index(lax.rem(pos + shift, n), n)
        there = held.at[pl.ds(origin * slots + first, size)]
        here = own.at[pl.ds(first, size)] if step == 0 else there
        return pltpu.make_async_remote_copy(
            src_ref=here,
            dst_ref=there,
            send_sem=send_sem.at[which, step, direction, j],
            recv_sem=recv_sem.at[which, step, direction, j],
            device_id={"fsdp": towards[direction]},
            device_id_type=pl.DeviceIdType.MESH,
        )

    def arrival(which, step, direction, j):
        first, size = parts[direction][j]
        own, held = arrays[which]
        shift = n - step - 1 if direction == 0 else step + 1
        origin = ring_index(lax.rem(pos + shift, n), n)
        there = held.at[pl.ds(origin * slots + first, size)]
        pltpu.make_async_remote_copy(
            src_ref=there,
            dst_ref=there,
            send_sem=send_sem.at[which, step, direction, j],
            recv_sem=recv_sem.at[which, step, direction, j],
            device_id={"fsdp": towards[direction]},
            device_id_type=pl.DeviceIdType.MESH,
        ).wait_recv()

    def each():
        for j in range(max(len(parts[0]), len(parts[1]))):
            for direction in range(2):
                if j < len(parts[direction]):
                    yield direction, j

    def normalize():
        rows = 32

        def some(i, carry):
            here = pl.ds(pl.multiple_of(i * rows, rows), rows)
            values = tokens_ref[here, :].astype(jnp.float32)
            factor = lax.rsqrt(jnp.mean(values * values, axis=-1, keepdims=True) + EPS)
            normed[here, :] = (values * factor * gain_ref[...]).astype(jnp.bfloat16)
            return carry

        lax.fori_loop(0, normed.shape[0] // rows, some, 0)

    def transpose():
        edge = held_w.shape[-1]

        def some(i, carry):
            here = pl.ds(pl.multiple_of(i * edge, edge), edge)
            normed_t_ref[here, :] = normed[:, here].T
            return carry

        lax.fori_loop(0, normed.shape[1] // edge, some, 0)

    def project(result_ref):
        rows = 256

        def some(i, carry):
            here = pl.ds(pl.multiple_of(i * rows, rows), rows)
            result_ref[here, :] = jnp.dot(
                normed[here, :], matrix[...], preferred_element_type=jnp.float32
            )
            return carry

        lax.fori_loop(0, normed.shape[0] // rows, some, 0)

    def unpack(which, qkv_ref, out_ref):
        own, held = arrays[which]
        rows, cols = grid_qkv
        edge = held.shape[-1]

        def qkv_row(i, carry):
            for c in range(cols):
                qkv_ref[pl.ds(pl.multiple_of(i * edge, edge), edge), c * edge:(c + 1) * edge] = (
                    held[slot_ref[i * cols + c]]
                )
            return carry

        lax.fori_loop(0, rows, qkv_row, 0)
        out_rows, out_cols = grid_out

        def out_col(i, carry):
            for r in range(out_rows):
                out_ref[r * edge:(r + 1) * edge, pl.ds(pl.multiple_of(i * edge, edge), edge)] = (
                    held[slot_ref[rows * cols + r * out_cols + i]]
                )
            return carry

        lax.fori_loop(0, out_cols, out_col, 0)

    def finish(which, qkv_ref, out_ref):
        own, held = arrays[which]
        for direction, j in each():
            arrival(which, n - 2, direction, j)
        held[pl.ds(me * slots, slots)] = own[...]
        unpack(which, qkv_ref, out_ref)

    sent = []
    for which in range(2):
        for step in range(n - 1):
            for direction, j in each():
                if step > 0:
                    arrival(which, step - 1, direction, j)
                one = copy(which, step, direction, j)
                one.start()
                sent.append(one)
            if which == 0 and step == 0:
                normalize()
            if which == 0 and step == 1:
                transpose()
            if which == 1 and step == 0:
                finish(0, matrix, wo_ref)
            if which == 1 and step == 1:
                project(proj_ref)
    finish(1, matrix, po_ref)
    project(d_proj_ref)
    for one in sent:
        one.wait_send()


def gather_weights(slot_of, weights, probes, tokens, gain, n, grid_qkv, grid_out):
    slots, edge, _ = weights.shape
    cuts = max(len(part) for part in pieces(slots))
    length, width = tokens.shape
    proj = jax.ShapeDtypeStruct((length, grid_qkv[1] * edge), jnp.float32)
    turned = jax.ShapeDtypeStruct((width, length), jnp.bfloat16)
    out = jax.ShapeDtypeStruct((grid_out[0] * edge, grid_out[1] * edge), jnp.bfloat16)
    vmem = pl.BlockSpec(memory_space=pltpu.VMEM)
    return pl.pallas_call(
        functools.partial(gather_kernel, n, slots, grid_qkv, grid_out),
        out_shape=(proj, proj, out, out, turned),
        in_specs=[pl.BlockSpec(memory_space=pltpu.SMEM)] + [vmem] * 4,
        out_specs=(vmem,) * 5,
        scratch_shapes=[
            pltpu.VMEM((n * slots, edge, edge), jnp.bfloat16),
            pltpu.VMEM((n * slots, edge, edge), jnp.bfloat16),
            pltpu.VMEM((grid_qkv[0] * edge, grid_qkv[1] * edge), jnp.bfloat16),
            pltpu.VMEM((length, width), jnp.bfloat16),
            pltpu.SemaphoreType.DMA((2, n - 1, 2, cuts)),
            pltpu.SemaphoreType.DMA((2, n - 1, 2, cuts)),
        ],
        compiler_params=pltpu.CompilerParams(
            collective_id=0, has_side_effects=True, vmem_limit_bytes=VMEM_BYTES
        ),
    )(slot_of, weights, probes, tokens, gain)


def gradient_kernel(grid_qkv, grid_out, slot_ref, normed_t_ref, d_proj_ref, mixed_t_ref,
                    weighted_ref, out_ref):
    edge = out_ref.shape[-1]
    rows, cols = grid_qkv
    out_rows, out_cols = grid_out
    group = 2

    def clear(i, carry):
        out_ref[i] = jnp.zeros(out_ref.shape[1:], out_ref.dtype)
        return carry

    lax.fori_loop(0, out_ref.shape[0], clear, 0)

    def qkv_rows(i, carry):
        width = group * edge
        left = normed_t_ref[pl.ds(pl.multiple_of(i * width, width), width), :]
        block = jnp.dot(
            left, d_proj_ref[...], preferred_element_type=jnp.float32
        ).astype(jnp.bfloat16)
        for r in range(group):
            for c in range(cols):
                out_ref[slot_ref[(i * group + r) * cols + c]] = block[
                    r * edge:(r + 1) * edge, c * edge:(c + 1) * edge
                ]
        return carry

    lax.fori_loop(0, rows // group, qkv_rows, 0)

    def out_columns(i, carry):
        width = group * edge
        right = weighted_ref[:, pl.ds(pl.multiple_of(i * width, width), width)]
        block = jnp.dot(
            mixed_t_ref[...], right, preferred_element_type=jnp.float32
        ).astype(jnp.bfloat16)
        for r in range(out_rows):
            for c in range(group):
                out_ref[slot_ref[rows * cols + r * out_cols + i * group + c]] = block[
                    r * edge:(r + 1) * edge, c * edge:(c + 1) * edge
                ]
        return carry

    lax.fori_loop(0, out_cols // group, out_columns, 0)


def gradient_slots(slot_of, normed_t, d_proj, mixed_t, weighted, total_slots, grid_qkv, grid_out):
    vmem = pl.BlockSpec(memory_space=pltpu.VMEM)
    return pl.pallas_call(
        functools.partial(gradient_kernel, grid_qkv, grid_out),
        out_shape=jax.ShapeDtypeStruct((total_slots, BLK, BLK), jnp.bfloat16),
        in_specs=[pl.BlockSpec(memory_space=pltpu.SMEM)] + [vmem] * 4,
        out_specs=vmem,
        compiler_params=pltpu.CompilerParams(vmem_limit_bytes=VMEM_BYTES),
    )(slot_of, normed_t, d_proj, mixed_t, weighted)


def reduce_kernel(n, slots, scale, g_ref, out_ref, held, send_sem, recv_sem):
    me = lax.axis_index("fsdp")
    pos = ring_position(me, n)
    right = ring_index(lax.rem(pos + 1, n), n)
    left = ring_index(lax.rem(pos + n - 1, n), n)
    towards = (right, left)
    enter((left, right))
    parts = pieces(slots)

    def own(step, direction, j):
        first, size = parts[direction][j]
        shift = n - 1 - step if direction == 0 else 1 + step
        target = ring_index(lax.rem(pos + shift, n), n)
        return pl.ds(target * slots + first, size)

    def copy(step, direction, j):
        first, size = parts[direction][j]
        here = g_ref.at[own(0, direction, j)] if step == 0 else held.at[step - 1, pl.ds(first, size)]
        return pltpu.make_async_remote_copy(
            src_ref=here,
            dst_ref=held.at[step, pl.ds(first, size)],
            send_sem=send_sem.at[step, direction, j],
            recv_sem=recv_sem.at[step, direction, j],
            device_id={"fsdp": towards[direction]},
            device_id_type=pl.DeviceIdType.MESH,
        )

    def each():
        for j in range(max(len(parts[0]), len(parts[1]))):
            for direction in range(2):
                if j < len(parts[direction]):
                    yield direction, j

    sent = {}
    for step in range(n - 1):
        for direction, j in each():
            first, size = parts[direction][j]
            if step > 0:
                sent[step - 1, direction, j].wait_recv()
                held[step - 1, pl.ds(first, size)] = (
                    held[step - 1, pl.ds(first, size)].astype(jnp.float32)
                    + g_ref[own(step, direction, j)].astype(jnp.float32)
                ).astype(jnp.bfloat16)
            one = copy(step, direction, j)
            one.start()
            sent[step, direction, j] = one
    for direction, j in each():
        first, size = parts[direction][j]
        sent[n - 2, direction, j].wait_recv()
        out_ref[pl.ds(first, size)] = (
            held[n - 2, pl.ds(first, size)].astype(jnp.float32)
            + g_ref[own(n - 1, direction, j)].astype(jnp.float32)
        ) * scale
    for one in sent.values():
        one.wait_send()


def reduce_slots(partial_slots, n, scale):
    total, edge, _ = partial_slots.shape
    slots = total // n
    cuts = max(len(part) for part in pieces(slots))
    vmem = pl.BlockSpec(memory_space=pltpu.VMEM)
    return pl.pallas_call(
        functools.partial(reduce_kernel, n, slots, scale),
        out_shape=jax.ShapeDtypeStruct((slots, edge, edge), jnp.float32),
        in_specs=[vmem],
        out_specs=vmem,
        scratch_shapes=[
            pltpu.VMEM((n - 1, slots, edge, edge), jnp.bfloat16),
            pltpu.SemaphoreType.DMA((n - 1, 2, cuts)),
            pltpu.SemaphoreType.DMA((n - 1, 2, cuts)),
        ],
        compiler_params=pltpu.CompilerParams(
            collective_id=1, has_side_effects=True, vmem_limit_bytes=VMEM_BYTES
        ),
    )(partial_slots)


def exchange_kernel(mixed_ref, d_mixed_ref, w_ref, p_ref, curv_ref, weighted_ref, back_ref,
                    terms, near, pair, far, share, rest, send_sem, recv_sem):
    me = lax.axis_index("seq")
    side = lax.rem(me, 2)
    core = me + 1 - 2 * side
    across = me + 2 - 4 * lax.rem(lax.div(me, 2), 2)
    enter((core, across), "seq")
    length, width = terms.shape
    half = width // 2
    chunks = recv_sem.shape[1]
    rows = length // chunks
    mine = pl.ds(pl.multiple_of(side * half, half), half)
    other = pl.ds(pl.multiple_of((1 - side) * half, half), half)

    def block(i):
        return pl.ds(i * rows, rows)

    def copy(stage, i, here, there, target):
        return pltpu.make_async_remote_copy(
            src_ref=here,
            dst_ref=there,
            send_sem=send_sem.at[stage, i],
            recv_sem=recv_sem.at[stage, i],
            device_id={"seq": target},
            device_id_type=pl.DeviceIdType.MESH,
        )

    def terms_of(i):
        tile = width // 4

        def columns(j, carry):
            cols = pl.ds(pl.multiple_of(j * tile, tile), tile)
            terms[block(i), cols] = (
                jnp.dot(d_mixed_ref[block(i), :], w_ref[:, cols], preferred_element_type=jnp.float32)
                + jnp.dot(mixed_ref[block(i), :], p_ref[:, cols], preferred_element_type=jnp.float32)
            ).astype(jnp.bfloat16)
            return carry

        lax.fori_loop(0, 4, columns, 0)

    first = [copy(0, i, terms.at[block(i), other], near.at[block(i)], core) for i in range(chunks)]
    second = [copy(1, i, pair.at[block(i)], far.at[block(i)], across) for i in range(chunks)]
    third = [copy(2, i, share.at[block(i)], rest.at[block(i)], core) for i in range(chunks)]

    def send_pair(i):
        first[i].wait_recv()
        pair[block(i)] = (
            terms[block(i), mine].astype(jnp.float32) + near[block(i)].astype(jnp.float32)
        ).astype(jnp.bfloat16)
        second[i].start()

    def send_share(i):
        second[i].wait_recv()
        total = pair[block(i)].astype(jnp.float32) + far[block(i)].astype(jnp.float32)
        share[block(i)] = (curv_ref[block(i), mine].astype(jnp.float32) * total).astype(
            jnp.bfloat16
        )
        third[i].start()

    def finish(i):
        weighted_ref[block(i), mine] = share[block(i)]
        third[i].wait_recv()
        weighted_ref[block(i), other] = rest[block(i)]
        back_ref[block(i), :] = lax.dot_general(
            weighted_ref[block(i), :],
            w_ref[...],
            (((1,), (1,)), ((), ())),
            preferred_element_type=jnp.float32,
        ).astype(jnp.bfloat16)

    for i in range(chunks):
        terms_of(i)
        first[i].start()
        if i > 0:
            send_pair(i - 1)
    send_pair(chunks - 1)
    for i in range(chunks):
        send_share(i)
        if i > 0:
            finish(i - 1)
    finish(chunks - 1)
    for one in first + second + third:
        one.wait_send()


def exchange(mixed, d_mixed, w_out, p_out, curvature):
    length, width = curvature.shape
    chunks = 4
    vmem = pl.BlockSpec(memory_space=pltpu.VMEM)
    half = pltpu.VMEM((length, width // 2), jnp.bfloat16)
    return pl.pallas_call(
        exchange_kernel,
        out_shape=(
            jax.ShapeDtypeStruct((length, width), jnp.bfloat16),
            jax.ShapeDtypeStruct(mixed.shape, jnp.bfloat16),
        ),
        in_specs=[vmem] * 5,
        out_specs=(vmem, vmem),
        scratch_shapes=[
            pltpu.VMEM((length, width), jnp.bfloat16),
            half,
            half,
            half,
            half,
            half,
            pltpu.SemaphoreType.DMA((3, chunks)),
            pltpu.SemaphoreType.DMA((3, chunks)),
        ],
        compiler_params=pltpu.CompilerParams(
            collective_id=2, has_side_effects=True, vmem_limit_bytes=VMEM_BYTES
        ),
    )(mixed, d_mixed, w_out, p_out, curvature)


def local(tokens, norm_gain, curvature, weight_slots, probe_slots, block_counts):
    n_columns = lax.axis_size("seq")
    n_owners = lax.axis_size("fsdp")
    q_heads = HQ // n_columns
    kv_heads = HK // n_columns
    row_blocks = D // BLK
    qkv_cols = (q_heads + 2 * kv_heads) * HD // BLK
    out_rows = q_heads * HD // BLK
    grid_qkv, grid_out = (row_blocks, qkv_cols), (out_rows, row_blocks)
    total_blocks = row_blocks * qkv_cols + out_rows * row_blocks
    slots = weight_slots.shape[1]
    length = tokens.shape[1]
    counts = block_counts[0]
    range_ends = jnp.cumsum(counts)
    starts = range_ends - counts
    owner_ids = jnp.arange(n_owners, dtype=jnp.int32)
    block_ids = jnp.arange(total_blocks, dtype=jnp.int32)
    owners = jnp.sum((range_ends[None, :] <= block_ids[:, None]).astype(jnp.int32), axis=1)
    first_block = jnp.sum(
        jnp.where(owners[:, None] == owner_ids[None, :], starts[None, :], 0), axis=1
    )
    slot_of = (owners * slots + block_ids - first_block).astype(jnp.int32)
    projected, d_projected, w_out, p_out, normed_t = gather_weights(
        slot_of,
        weight_slots[0],
        probe_slots[0],
        tokens[0],
        norm_gain[None, :],
        n_owners,
        grid_qkv,
        grid_out,
    )
    cosine, sine = rotary(length, HD)

    def inner(projected):
        return attention(projected, cosine, sine, q_heads, kv_heads)

    mixed, d_mixed = jax.jvp(inner, (projected,), (d_projected,))
    weighted, back_mixed = exchange(mixed, d_mixed, w_out, p_out, curvature[0])
    mixed_again, pullback = jax.vjp(inner, projected)
    (back_projected,) = pullback(back_mixed)
    partial_slots = gradient_slots(
        slot_of,
        normed_t,
        back_projected.astype(jnp.bfloat16),
        mixed_again.T,
        weighted,
        n_owners * slots,
        grid_qkv,
        grid_out,
    )
    scaled = reduce_slots(partial_slots, n_owners, (length * n_owners) ** -0.5)
    return scaled.reshape(1, slots, BLK, BLK)


def solution(mesh):
    in_specs = (
        P("fsdp", None, None),
        P(),
        P("fsdp", None, None),
        P("seq", "fsdp", None, None),
        P("seq", "fsdp", None, None),
        P("seq", None),
    )
    out_specs = P("seq", "fsdp", None, None)
    return jax.shard_map(local, mesh=mesh, in_specs=in_specs, out_specs=out_specs, check_vma=False)
```

```python
import functools

import jax
import jax.numpy as jnp
from jax import lax
from jax.experimental import pallas as pl
from jax.experimental.pallas import tpu as pltpu
from jax.sharding import PartitionSpec as P

D = 4096
HQ = 16
HK = 4
HD = 128
BLK = 128


THETA = 500000.0
EPS = 1e-05
NEGATIVE = -1e30


def rotary(length, head_dim):
    half_dim = head_dim // 2
    frequency = jnp.exp(-jnp.log(THETA) * 2.0 * jnp.arange(half_dim, dtype=jnp.float32) / head_dim)
    angles = jnp.arange(length, dtype=jnp.float32)[:, None] * frequency[None, :]
    return (jnp.cos(angles)[:, None, :], jnp.sin(angles)[:, None, :])


def rotate(field_in, cosine, sine):
    half_dim = field_in.shape[-1] // 2
    first_half = field_in[..., :half_dim]
    second = field_in[..., half_dim:]
    return jnp.concatenate(
        [first_half * cosine - second * sine, second * cosine + first_half * sine], axis=-1
    )


VMEM_BYTES = 62 * 1024 * 1024


def attention(projected, cosine, sine, q_heads, kv_heads):
    length = projected.shape[0]
    head_dim = projected.shape[1] // (q_heads + 2 * kv_heads)
    q_end = q_heads * head_dim
    k_end = q_end + kv_heads * head_dim
    queries = rotate(projected[:, :q_end].reshape(length, q_heads, head_dim), cosine, sine).astype(
        jnp.bfloat16
    )
    key_rows = rotate(
        projected[:, q_end:k_end].reshape(length, kv_heads, head_dim), cosine, sine
    ).astype(jnp.bfloat16)
    values = projected[:, k_end:].reshape(length, kv_heads, head_dim).astype(jnp.bfloat16)
    queries = queries.reshape(length, kv_heads, q_heads // kv_heads, head_dim)
    scores = jnp.einsum(
        "qkgd,skd->kgqs", queries, key_rows, preferred_element_type=jnp.float32
    ) * head_dim ** (-0.5)
    causal = jnp.arange(length)[:, None] >= jnp.arange(length)[None, :]
    scores = jnp.where(causal, scores, NEGATIVE)
    attn_probs = jax.nn.softmax(scores, axis=-1).astype(jnp.bfloat16)
    mixed_heads = jnp.einsum(
        "kgqs,skd->qkgd", attn_probs, values, preferred_element_type=jnp.float32
    )
    return mixed_heads.reshape(length, q_heads * head_dim).astype(jnp.bfloat16)


def ring_position(index, n):
    odd = lax.rem(index, 2)
    half = lax.div(index, 2)
    return (1 - odd) * half + odd * (n - 1 - half)


def ring_index(position, n):
    back = lax.div(position, n // 2)
    return (1 - back) * 2 * position + back * (2 * (n - 1 - position) + 1)


def pieces(slots):
    half = slots // 2
    out = []
    for direction, first, count in ((0, 0, half), (1, half, slots - half)):
        cuts = 5 if count % 5 == 0 else 1
        size = count // cuts
        out.append([(first + i * size, size) for i in range(cuts)])
    return out


def enter(neighbours, axis="fsdp"):
    barrier = pltpu.get_barrier_semaphore()
    for neighbour in neighbours:
        pl.semaphore_signal(
            barrier, inc=1, device_id={axis: neighbour}, device_id_type=pl.DeviceIdType.MESH
        )
    pl.semaphore_wait(barrier, len(neighbours))


def gather_kernel(n, slots, grid_qkv, grid_out, slot_ref, w_ref, p_ref, tokens_ref, gain_ref,
                  proj_ref, d_proj_ref, wo_ref, po_ref, normed_t_ref, held_w, held_p, matrix,
                  normed, send_sem, recv_sem):
    me = lax.axis_index("fsdp")
    pos = ring_position(me, n)
    right = ring_index(lax.rem(pos + 1, n), n)
    left = ring_index(lax.rem(pos + n - 1, n), n)
    towards = (right, left)
    enter((left, right))
    parts = pieces(slots)
    arrays = ((w_ref, held_w), (p_ref, held_p))

    def copy(which, step, direction, j):
        own, held = arrays[which]
        first, size = parts[direction][j]
        shift = n - step if direction == 0 else step
        origin = ring_index(lax.rem(pos + shift, n), n)
        there = held.at[pl.ds(origin * slots + first, size)]
        here = own.at[pl.ds(first, size)] if step == 0 else there
        return pltpu.make_async_remote_copy(
            src_ref=here,
            dst_ref=there,
            send_sem=send_sem.at[which, step, direction, j],
            recv_sem=recv_sem.at[which, step, direction, j],
            device_id={"fsdp": towards[direction]},
            device_id_type=pl.DeviceIdType.MESH,
        )

    def arrival(which, step, direction, j):
        first, size = parts[direction][j]
        own, held = arrays[which]
        shift = n - step - 1 if direction == 0 else step + 1
        origin = ring_index(lax.rem(pos + shift, n), n)
        there = held.at[pl.ds(origin * slots + first, size)]
        pltpu.make_async_remote_copy(
            src_ref=there,
            dst_ref=there,
            send_sem=send_sem.at[which, step, direction, j],
            recv_sem=recv_sem.at[which, step, direction, j],
            device_id={"fsdp": towards[direction]},
            device_id_type=pl.DeviceIdType.MESH,
        ).wait_recv()

    def each():
        for j in range(max(len(parts[0]), len(parts[1]))):
            for direction in range(2):
                if j < len(parts[direction]):
                    yield direction, j

    def normalize():
        rows = 32

        def some(i, carry):
            here = pl.ds(pl.multiple_of(i * rows, rows), rows)
            values = tokens_ref[here, :].astype(jnp.float32)
            factor = lax.rsqrt(jnp.mean(values * values, axis=-1, keepdims=True) + EPS)
            normed[here, :] = (values * factor * gain_ref[...]).astype(jnp.bfloat16)
            return carry

        lax.fori_loop(0, normed.shape[0] // rows, some, 0)

    def transpose():
        edge = held_w.shape[-1]

        def some(i, carry):
            here = pl.ds(pl.multiple_of(i * edge, edge), edge)
            normed_t_ref[here, :] = normed[:, here].T
            return carry

        lax.fori_loop(0, normed.shape[1] // edge, some, 0)

    def project(result_ref):
        rows = 256

        def some(i, carry):
            here = pl.ds(pl.multiple_of(i * rows, rows), rows)
            result_ref[here, :] = jnp.dot(
                normed[here, :], matrix[...], preferred_element_type=jnp.float32
            )
            return carry

        lax.fori_loop(0, normed.shape[0] // rows, some, 0)

    def unpack(which, qkv_ref, out_ref):
        own, held = arrays[which]
        rows, cols = grid_qkv
        edge = held.shape[-1]

        def qkv_row(i, carry):
            for c in range(cols):
                qkv_ref[pl.ds(pl.multiple_of(i * edge, edge), edge), c * edge:(c + 1) * edge] = (
                    held[slot_ref[i * cols + c]]
                )
            return carry

        lax.fori_loop(0, rows, qkv_row, 0)
        out_rows, out_cols = grid_out

        def out_col(i, carry):
            for r in range(out_rows):
                out_ref[r * edge:(r + 1) * edge, pl.ds(pl.multiple_of(i * edge, edge), edge)] = (
                    held[slot_ref[rows * cols + r * out_cols + i]]
                )
            return carry

        lax.fori_loop(0, out_cols, out_col, 0)

    def finish(which, qkv_ref, out_ref):
        own, held = arrays[which]
        for direction, j in each():
            arrival(which, n - 2, direction, j)
        held[pl.ds(me * slots, slots)] = own[...]
        unpack(which, qkv_ref, out_ref)

    sent = []
    for which in range(2):
        for step in range(n - 1):
            for direction, j in each():
                if step > 0:
                    arrival(which, step - 1, direction, j)
                one = copy(which, step, direction, j)
                one.start()
                sent.append(one)
            if which == 0 and step == 0:
                normalize()
            if which == 0 and step == 1:
                transpose()
            if which == 1 and step == 0:
                finish(0, matrix, wo_ref)
            if which == 1 and step == 1:
                project(proj_ref)
    finish(1, matrix, po_ref)
    project(d_proj_ref)
    for one in sent:
        one.wait_send()


def gather_weights(slot_of, weights, probes, tokens, gain, n, grid_qkv, grid_out):
    slots, edge, _ = weights.shape
    cuts = max(len(part) for part in pieces(slots))
    length, width = tokens.shape
    proj = jax.ShapeDtypeStruct((length, grid_qkv[1] * edge), jnp.float32)
    turned = jax.ShapeDtypeStruct((width, length), jnp.bfloat16)
    out = jax.ShapeDtypeStruct((grid_out[0] * edge, grid_out[1] * edge), jnp.bfloat16)
    vmem = pl.BlockSpec(memory_space=pltpu.VMEM)
    return pl.pallas_call(
        functools.partial(gather_kernel, n, slots, grid_qkv, grid_out),
        out_shape=(proj, proj, out, out, turned),
        in_specs=[pl.BlockSpec(memory_space=pltpu.SMEM)] + [vmem] * 4,
        out_specs=(vmem,) * 5,
        scratch_shapes=[
            pltpu.VMEM((n * slots, edge, edge), jnp.bfloat16),
            pltpu.VMEM((n * slots, edge, edge), jnp.bfloat16),
            pltpu.VMEM((grid_qkv[0] * edge, grid_qkv[1] * edge), jnp.bfloat16),
            pltpu.VMEM((length, width), jnp.bfloat16),
            pltpu.SemaphoreType.DMA((2, n - 1, 2, cuts)),
            pltpu.SemaphoreType.DMA((2, n - 1, 2, cuts)),
        ],
        compiler_params=pltpu.CompilerParams(
            collective_id=0, has_side_effects=True, vmem_limit_bytes=VMEM_BYTES
        ),
    )(slot_of, weights, probes, tokens, gain)


def gradient_blocks(grid_qkv, grid_out, normed_t_ref, d_proj_ref, mixed_t_ref, weighted_ref,
                    out_ref):
    edge = out_ref.shape[-1]
    rows, cols = grid_qkv
    out_rows, out_cols = grid_out
    group = 2

    out_ref[rows * cols + out_rows * out_cols] = jnp.zeros((edge, edge), out_ref.dtype)

    def qkv_rows(i, carry):
        width = group * edge
        left = normed_t_ref[pl.ds(pl.multiple_of(i * width, width), width), :]
        block = jnp.dot(
            left, d_proj_ref[...], preferred_element_type=jnp.float32
        ).astype(jnp.bfloat16)
        for r in range(group):
            for c in range(cols):
                out_ref[(i * group + r) * cols + c] = block[
                    r * edge:(r + 1) * edge, c * edge:(c + 1) * edge
                ]
        return carry

    lax.fori_loop(0, rows // group, qkv_rows, 0)

    def out_columns(i, carry):
        width = group * edge
        right = weighted_ref[:, pl.ds(pl.multiple_of(i * width, width), width)]
        block = jnp.dot(
            mixed_t_ref[...], right, preferred_element_type=jnp.float32
        ).astype(jnp.bfloat16)
        for r in range(out_rows):
            for c in range(group):
                out_ref[rows * cols + r * out_cols + i * group + c] = block[
                    r * edge:(r + 1) * edge, c * edge:(c + 1) * edge
                ]
        return carry

    lax.fori_loop(0, out_cols // group, out_columns, 0)


def reduce_kernel(n, slots, scale, grid_qkv, grid_out, pick_ref, normed_t_ref, d_proj_ref,
                  mixed_t_ref, weighted_ref, out_ref, grads, begin, held, send_sem, recv_sem):
    me = lax.axis_index("fsdp")
    pos = ring_position(me, n)
    right = ring_index(lax.rem(pos + 1, n), n)
    left = ring_index(lax.rem(pos + n - 1, n), n)
    towards = (right, left)
    enter((left, right))
    parts = pieces(slots)
    gradient_blocks(
        grid_qkv, grid_out, normed_t_ref, d_proj_ref, mixed_t_ref, weighted_ref, grads
    )

    def own(step, direction, j):
        shift = n - 1 - step if direction == 0 else 1 + step
        target = ring_index(lax.rem(pos + shift, n), n)
        return target * slots

    def each_block(direction, j, body):
        first, size = parts[direction][j]

        def some(i, carry):
            body(first + i)
            return carry

        lax.fori_loop(0, size, some, 0)

    def copy(step, direction, j):
        first, size = parts[direction][j]
        here = begin.at[pl.ds(first, size)] if step == 0 else held.at[step - 1, pl.ds(first, size)]
        return pltpu.make_async_remote_copy(
            src_ref=here,
            dst_ref=held.at[step, pl.ds(first, size)],
            send_sem=send_sem.at[step, direction, j],
            recv_sem=recv_sem.at[step, direction, j],
            device_id={"fsdp": towards[direction]},
            device_id_type=pl.DeviceIdType.MESH,
        )

    def each():
        for j in range(max(len(parts[0]), len(parts[1]))):
            for direction in range(2):
                if j < len(parts[direction]):
                    yield direction, j

    sent = {}
    for step in range(n - 1):
        for direction, j in each():
            first, size = parts[direction][j]
            base = own(step, direction, j)
            if step > 0:
                sent[step - 1, direction, j].wait_recv()

                def add(t, step=step, base=base):
                    held[step - 1, t] = (
                        held[step - 1, t].astype(jnp.float32)
                        + grads[pick_ref[base + t]].astype(jnp.float32)
                    ).astype(jnp.bfloat16)

                each_block(direction, j, add)
            else:

                def fill(t, base=base):
                    begin[t] = grads[pick_ref[base + t]]

                each_block(direction, j, fill)
            one = copy(step, direction, j)
            one.start()
            sent[step, direction, j] = one
    for direction, j in each():
        first, size = parts[direction][j]
        sent[n - 2, direction, j].wait_recv()
        base = own(n - 1, direction, j)

        def last(t, base=base):
            out_ref[t] = (
                held[n - 2, t].astype(jnp.float32) + grads[pick_ref[base + t]].astype(jnp.float32)
            ) * scale

        each_block(direction, j, last)
    for one in sent.values():
        one.wait_send()


def reduce_slots(picked, normed_t, d_proj, mixed_t, weighted, n, scale, grid_qkv, grid_out):
    slots = picked.shape[0] // n
    edge = BLK
    total_blocks = grid_qkv[0] * grid_qkv[1] + grid_out[0] * grid_out[1]
    cuts = max(len(part) for part in pieces(slots))
    vmem = pl.BlockSpec(memory_space=pltpu.VMEM)
    return pl.pallas_call(
        functools.partial(reduce_kernel, n, slots, scale, grid_qkv, grid_out),
        out_shape=jax.ShapeDtypeStruct((slots, edge, edge), jnp.float32),
        in_specs=[pl.BlockSpec(memory_space=pltpu.SMEM)] + [vmem] * 4,
        out_specs=vmem,
        scratch_shapes=[
            pltpu.VMEM((total_blocks + 1, edge, edge), jnp.bfloat16),
            pltpu.VMEM((slots, edge, edge), jnp.bfloat16),
            pltpu.VMEM((n - 1, slots, edge, edge), jnp.bfloat16),
            pltpu.SemaphoreType.DMA((n - 1, 2, cuts)),
            pltpu.SemaphoreType.DMA((n - 1, 2, cuts)),
        ],
        compiler_params=pltpu.CompilerParams(
            collective_id=1, has_side_effects=True, vmem_limit_bytes=VMEM_BYTES
        ),
    )(picked, normed_t, d_proj, mixed_t, weighted)


def exchange_kernel(mixed_ref, d_mixed_ref, w_ref, p_ref, curv_ref, weighted_ref, back_ref,
                    terms, near, pair, far, share, rest, send_sem, recv_sem):
    me = lax.axis_index("seq")
    side = lax.rem(me, 2)
    core = me + 1 - 2 * side
    across = me + 2 - 4 * lax.rem(lax.div(me, 2), 2)
    enter((core, across), "seq")
    length, width = terms.shape
    half = width // 2
    chunks = recv_sem.shape[1]
    rows = length // chunks
    mine = pl.ds(pl.multiple_of(side * half, half), half)
    other = pl.ds(pl.multiple_of((1 - side) * half, half), half)

    def block(i):
        return pl.ds(i * rows, rows)

    def copy(stage, i, here, there, target):
        return pltpu.make_async_remote_copy(
            src_ref=here,
            dst_ref=there,
            send_sem=send_sem.at[stage, i],
            recv_sem=recv_sem.at[stage, i],
            device_id={"seq": target},
            device_id_type=pl.DeviceIdType.MESH,
        )

    def terms_of(i):
        tile = width // 4

        def columns(j, carry):
            cols = pl.ds(pl.multiple_of(j * tile, tile), tile)
            terms[block(i), cols] = (
                jnp.dot(d_mixed_ref[block(i), :], w_ref[:, cols], preferred_element_type=jnp.float32)
                + jnp.dot(mixed_ref[block(i), :], p_ref[:, cols], preferred_element_type=jnp.float32)
            ).astype(jnp.bfloat16)
            return carry

        lax.fori_loop(0, 4, columns, 0)

    first = [copy(0, i, terms.at[block(i), other], near.at[block(i)], core) for i in range(chunks)]
    second = [copy(1, i, pair.at[block(i)], far.at[block(i)], across) for i in range(chunks)]
    third = [copy(2, i, share.at[block(i)], rest.at[block(i)], core) for i in range(chunks)]

    def send_pair(i):
        first[i].wait_recv()
        pair[block(i)] = (
            terms[block(i), mine].astype(jnp.float32) + near[block(i)].astype(jnp.float32)
        ).astype(jnp.bfloat16)
        second[i].start()

    def send_share(i):
        second[i].wait_recv()
        total = pair[block(i)].astype(jnp.float32) + far[block(i)].astype(jnp.float32)
        share[block(i)] = (curv_ref[block(i), mine].astype(jnp.float32) * total).astype(
            jnp.bfloat16
        )
        third[i].start()

    def finish(i):
        weighted_ref[block(i), mine] = share[block(i)]
        third[i].wait_recv()
        weighted_ref[block(i), other] = rest[block(i)]
        back_ref[block(i), :] = lax.dot_general(
            weighted_ref[block(i), :],
            w_ref[...],
            (((1,), (1,)), ((), ())),
            preferred_element_type=jnp.float32,
        ).astype(jnp.bfloat16)

    for i in range(chunks):
        terms_of(i)
        first[i].start()
        if i > 0:
            send_pair(i - 1)
    send_pair(chunks - 1)
    for i in range(chunks):
        send_share(i)
        if i > 0:
            finish(i - 1)
    finish(chunks - 1)
    for one in first + second + third:
        one.wait_send()


def exchange(mixed, d_mixed, w_out, p_out, curvature):
    length, width = curvature.shape
    chunks = 4
    vmem = pl.BlockSpec(memory_space=pltpu.VMEM)
    half = pltpu.VMEM((length, width // 2), jnp.bfloat16)
    return pl.pallas_call(
        exchange_kernel,
        out_shape=(
            jax.ShapeDtypeStruct((length, width), jnp.bfloat16),
            jax.ShapeDtypeStruct(mixed.shape, jnp.bfloat16),
        ),
        in_specs=[vmem] * 5,
        out_specs=(vmem, vmem),
        scratch_shapes=[
            pltpu.VMEM((length, width), jnp.bfloat16),
            half,
            half,
            half,
            half,
            half,
            pltpu.SemaphoreType.DMA((3, chunks)),
            pltpu.SemaphoreType.DMA((3, chunks)),
        ],
        compiler_params=pltpu.CompilerParams(
            collective_id=2, has_side_effects=True, vmem_limit_bytes=VMEM_BYTES
        ),
    )(mixed, d_mixed, w_out, p_out, curvature)


def local(tokens, norm_gain, curvature, weight_slots, probe_slots, block_counts):
    n_columns = lax.axis_size("seq")
    n_owners = lax.axis_size("fsdp")
    q_heads = HQ // n_columns
    kv_heads = HK // n_columns
    row_blocks = D // BLK
    qkv_cols = (q_heads + 2 * kv_heads) * HD // BLK
    out_rows = q_heads * HD // BLK
    grid_qkv, grid_out = (row_blocks, qkv_cols), (out_rows, row_blocks)
    total_blocks = row_blocks * qkv_cols + out_rows * row_blocks
    slots = weight_slots.shape[1]
    length = tokens.shape[1]
    counts = block_counts[0]
    range_ends = jnp.cumsum(counts)
    starts = range_ends - counts
    owner_ids = jnp.arange(n_owners, dtype=jnp.int32)
    block_ids = jnp.arange(total_blocks, dtype=jnp.int32)
    owners = jnp.sum((range_ends[None, :] <= block_ids[:, None]).astype(jnp.int32), axis=1)
    first_block = jnp.sum(
        jnp.where(owners[:, None] == owner_ids[None, :], starts[None, :], 0), axis=1
    )
    slot_of = (owners * slots + block_ids - first_block).astype(jnp.int32)
    projected, d_projected, w_out, p_out, normed_t = gather_weights(
        slot_of,
        weight_slots[0],
        probe_slots[0],
        tokens[0],
        norm_gain[None, :],
        n_owners,
        grid_qkv,
        grid_out,
    )
    cosine, sine = rotary(length, HD)

    def inner(projected):
        return attention(projected, cosine, sine, q_heads, kv_heads)

    mixed, d_mixed = jax.jvp(inner, (projected,), (d_projected,))
    weighted, back_mixed = exchange(mixed, d_mixed, w_out, p_out, curvature[0])
    mixed_again, pullback = jax.vjp(inner, projected)
    (back_projected,) = pullback(back_mixed)
    slot_index = jnp.arange(n_owners * slots, dtype=jnp.int32)
    place = slot_index % slots
    owner_hot = (slot_index // slots)[:, None] == owner_ids[None, :]
    owner_first = jnp.sum(jnp.where(owner_hot, starts[None, :], 0), axis=1)
    own_count = jnp.sum(jnp.where(owner_hot, counts[None, :], 0), axis=1)
    picked = jnp.where(place < own_count, owner_first + place, total_blocks).astype(jnp.int32)
    scaled = reduce_slots(
        picked,
        normed_t,
        back_projected.astype(jnp.bfloat16),
        mixed_again.T,
        weighted,
        n_owners,
        (length * n_owners) ** -0.5,
        grid_qkv,
        grid_out,
    )
    return scaled.reshape(1, slots, BLK, BLK)


def solution(mesh):
    in_specs = (
        P("fsdp", None, None),
        P(),
        P("fsdp", None, None),
        P("seq", "fsdp", None, None),
        P("seq", "fsdp", None, None),
        P("seq", None),
    )
    out_specs = P("seq", "fsdp", None, None)
    return jax.shard_map(local, mesh=mesh, in_specs=in_specs, out_specs=out_specs, check_vma=False)
```
